32 devices in a mesh: dp: 4 (over x, y), sp: 8 (over z, core).
Axes of the slice: x: 2, y: 2, z: 4, core: 2. Of those that a mesh axis runs over, the one named last changes fastest.
Arguments:
- q: bfloat16 [128, 96, 128], P('dp'), parts along dimension 0
- k: bfloat16 [128, 8192, 8, 128], P('dp', 'sp'), parts along dimension 0
- v: bfloat16 [128, 8192, 8, 128], P('dp', 'sp'), parts along dimension 0
Outputs:
- q: bfloat16 [128, 96, 128], P('dp'), parts along dimension 0
There are 4 independent parts. The reference program is written for one: setup_inputs(seed, part) draws one part's arguments, and reference() takes and returns one part's arrays. A program takes and returns all parts, laid end to end along the dimension named above; each array names one.
All inputs are finite; a program needn't handle non-finite values.
Results may differ from the reference program's by a relative error of at most 0.012.
Values are sent between devices in bfloat16 or wider.
A program may use at most 2 GiB of HBM per device.

```python
import jax
import jax.numpy as jnp

BATCH = 32
CACHE = 8192
HEADS = 96
KV_HEADS = 8
HEAD = 128


def setup_inputs(seed: int = 0, part: int = 0) -> dict:
    kq, kk, kv = (jax.random.fold_in(k, part) for k in jax.random.split(jax.random.key(seed), 3))
    return {
        "q": (3 * jax.random.normal(kq, (BATCH, HEADS, HEAD), jnp.float32)).astype(jnp.bfloat16),
        "k": jax.random.normal(kk, (BATCH, CACHE, KV_HEADS, HEAD), jnp.float32).astype(jnp.bfloat16),
        "v": jax.random.normal(kv, (BATCH, CACHE, KV_HEADS, HEAD), jnp.float32).astype(jnp.bfloat16),
    }


def einsum(form, a, b):
    return jnp.einsum(form, a.astype(jnp.float32), b.astype(jnp.float32))


def reference(q, k, v):
    grouped = q.reshape(BATCH, KV_HEADS, -1, HEAD)
    scores = einsum("bgsd,bugd->bgsu", grouped, k) * HEAD**-0.5
    weights = jax.nn.softmax(scores, -1).astype(jnp.bfloat16)
    return einsum("bgsu,bugd->bgsd", weights, v).astype(jnp.bfloat16).reshape(BATCH, HEADS, HEAD)
```

```python
import functools

import jax
import jax.numpy as jnp
from jax import lax
from jax.experimental import pallas as pl
from jax.experimental.pallas import tpu as pltpu
from jax.sharding import PartitionSpec as P

F32, BF16 = jnp.float32, jnp.bfloat16
LOG2E = 1.4426950408889634
GROUP = 16
STEP = 4
CHUNK = 512


def place(rows, cols, wide, given):
    r = lax.broadcasted_iota(jnp.int32, (rows, cols), 0)
    c = lax.broadcasted_iota(jnp.int32, (rows, cols), 1)
    return jnp.where((r % wide < given) & (c == r // wide * given + r % wide), 1.0, 0.0).astype(BF16)


def take(rows, cols, wide, given):
    r = lax.broadcasted_iota(jnp.int32, (rows, cols), 0)
    c = lax.broadcasted_iota(jnp.int32, (rows, cols), 1)
    return jnp.where((c % wide < given) & (r == c // wide * given + c % wide), 1.0, 0.0).astype(BF16)


def classes(x, heads, f):
    step = heads
    while step < 128:
        x = f(x, pltpu.roll(x, step, 1))
        step *= 2
    return x


def kernel(n, heads, devices, q_ref, k_hbm, v_hbm, out, *scratch):
    kb, vb = scratch[:STEP], scratch[STEP : 2 * STEP]
    (qq, r_ref, mx, pm, pmt, px, pxt, obuf, sbuf, orecv, srecv, fbuf) = scratch[2 * STEP : 2 * STEP + 12]
    (ksem, vsem, o_send, s_send, o_recv, s_recv, f_send, f_recv, f_own) = scratch[2 * STEP + 12 :]
    rows = k_hbm.shape[1]
    half = rows // 2
    total = heads * GROUP
    given = q_ref.shape[1] // heads
    part = q_ref.shape[1] // 2
    scale = q_ref.shape[2] ** -0.5 * LOG2E
    steps = n // STEP
    me = lax.axis_index("sp")
    chip, core = me // 2, me % 2
    mine = (chip + STEP - 1) % STEP

    lane = lax.broadcasted_iota(jnp.int32, (GROUP, 128), 1)
    masks = [lane % heads == h for h in range(heads)]
    keep = [m.astype(F32).astype(BF16) for m in masks]
    lane8 = lane[:8]

    def kcopy(u, i):
        return pltpu.make_async_copy(k_hbm.at[jnp.minimum(i * STEP + u, n - 1)], kb[u].at[i % 2], ksem.at[u, i % 2])

    def vcopy(u, i):
        return pltpu.make_async_copy(v_hbm.at[jnp.minimum(i * STEP + u, n - 1)], vb[u].at[i % 2], vsem.at[u, i % 2])

    def o_copy(b, d):
        peer = (me + d) % devices
        turn = (peer // 2 + STEP - 1) % STEP
        return pltpu.make_async_remote_copy(
            obuf.at[b, turn, peer % 2], orecv.at[b + 2, d], o_send.at[b, d], o_recv.at[b, d], device_id={"sp": peer}
        )

    def s_copy(b, d):
        peer = (me + d) % devices
        turn = (peer // 2 + STEP - 1) % STEP
        return pltpu.make_async_remote_copy(
            sbuf.at[b, turn], srecv.at[b + 2, d], s_send.at[b, d], s_recv.at[b, d], device_id={"sp": peer}
        )

    def f_copy(b, d):
        peer = (me + d) % devices
        return pltpu.make_async_remote_copy(
            fbuf.at[b + 2], out.at[jnp.minimum(b * STEP + mine, n), core], f_send.at[b, d], f_recv.at[b, d], device_id={"sp": peer}
        )

    def f_local(b):
        return pltpu.make_async_copy(fbuf.at[b + 2], out.at[jnp.minimum(b * STEP + mine, n), core], f_own.at[b])

    others = range(1, devices)

    def send_parts(b):
        for d in others:
            o_copy(b, d).start()
            s_copy(b, d).start()

    def wait_parts(b):
        for d in others:
            o_copy(b, d).wait_recv()
            s_copy(b, d).wait_recv()

    def sent_parts(b):
        for d in others:
            o_copy(b, d).wait_send()
            s_copy(b, d).wait_send()

    def send_result(b):
        f_local(b).start()
        for d in others:
            f_copy(b, d).start()

    def done_result(b):
        f_local(b).wait()
        for d in others:
            f_copy(b, d).wait_send()
            f_copy(b, d).wait_recv()

    def combine(b):
        own = jnp.maximum(b, 0)
        stats = [sbuf[own, mine]] + [srecv[b + 2, d] for d in others]
        parts = [obuf[own, mine, core]] + [orecv[b + 2, d] for d in others]
        high = functools.reduce(jnp.maximum, stats)
        scales = [jnp.exp2((s - high) * scale) for s in stats]
        below = functools.reduce(jnp.add, [a * pltpu.roll(s, 128 - heads, 1) for a, s in zip(scales, stats)])
        inverse = 1.0 / below
        wide = jnp.dot(px[...], jnp.concatenate(parts, 1), preferred_element_type=F32)
        sums = jnp.zeros((total // 2, 128), F32)
        for d, a in enumerate(scales):
            w = a * inverse
            w = jnp.where(core == 0, w, pltpu.roll(w, 128 - heads // 2, 1))
            spread = jnp.concatenate(
                [
                    jnp.broadcast_to(w[:, 64 * (e % 2) + e // 2 : 64 * (e % 2) + e // 2 + 1], (8, 128))
                    for e in range(heads)
                ],
                0,
            )
            sums = sums + wide[:, d * 128 : (d + 1) * 128] * spread
        fbuf[b + 2] = jnp.dot(pxt[...], sums.astype(BF16), preferred_element_type=F32).astype(BF16)

    def values(high, source, v, b, u):
        base = high * scale
        seen = jnp.zeros((2 * total, 256), F32)
        sums = jnp.zeros((GROUP, 128), F32)
        t = CHUNK // 128 if half >= CHUNK else half // 128
        size = t * 128
        for c in range(half // size):
            parts = []
            for side in range(2):
                for x in range(t):
                    p = jnp.exp2(r_ref[source, side, :, pl.ds(c * size + x * 128, 128)] * scale - base)
                    sums = sums + p
                    parts.append(p.astype(BF16))
            spread = jnp.concatenate(
                [
                    jnp.concatenate([parts[side * t + x] * keep[h] for x in range(t)], 1)
                    for side in range(2)
                    for h in range(heads)
                ],
                0,
            )
            vv = jnp.concatenate([v[pl.ds(c * size, size)], v[pl.ds(half + c * size, size)]], 1)
            seen = seen + jnp.dot(spread, vv, preferred_element_type=F32)
            yield
        sums = classes(sums, heads, jnp.add)
        o = (seen[:total, :128] + seen[total:, 128:]).astype(BF16)
        o = jnp.dot(pmt[...], o, preferred_element_type=F32).astype(BF16)
        obuf[b, u, 0] = o[:part]
        obuf[b, u, 1] = o[part:]
        first = lane8 // heads % 2 == 0
        low = jnp.where(first, high[:8], sums[:8])
        high = jnp.where(first, high[8:], sums[8:])
        sbuf[b, u] = jnp.where(lane8 < 64, low, high)
        yield

    def scores(query, target, k, best):
        t = CHUNK // 128 if half >= CHUNK else half // 128
        size = t * 128
        for c in range(half // size):
            kk = jnp.concatenate([k[pl.ds(c * size, size)], k[pl.ds(half + c * size, size)]], 1)
            s = lax.dot_general(query, kk, (((1,), (1,)), ((), ())), preferred_element_type=F32)
            for side in range(2):
                for x in range(t):
                    cols = slice(x * 128, (x + 1) * 128)
                    r = s[side * total : side * total + GROUP, cols]
                    for h in range(1, heads):
                        first = side * total + h * GROUP
                        r = jnp.where(masks[h], s[first : first + GROUP, cols], r)
                    r_ref[target, side, :, pl.ds(c * size + x * 128, 128)] = r
                    best[0] = jnp.maximum(best[0], r)
            yield

    for i in range(2):
        for u in range(STEP):
            kcopy(u, i).start()
            if (i, u) != (1, STEP - 1):
                vcopy(u, i).start()

    barrier = pltpu.get_barrier_semaphore()
    for d in others:
        pl.semaphore_signal(barrier, inc=1, device_id={"sp": (me + d) % devices})
    pl.semaphore_wait(barrier, devices - 1)

    pm[...] = place(total, q_ref.shape[1], GROUP, given)
    pmt[...] = take(q_ref.shape[1], total, GROUP, given)
    px[...] = place(total // 2, part, GROUP, given)
    pxt[...] = take(part, total // 2, GROUP, given)
    qq[...] = jnp.zeros_like(qq)
    r_ref[...] = jnp.zeros_like(r_ref)
    mx[...] = jnp.zeros_like(mx)

    def step(i, _):
        @pl.when(i >= 1)
        def _():
            send_parts(i - 1)
            vcopy(STEP - 1, i - 1).wait()

        @pl.when(i >= 3)
        def _():
            send_result(i - 3)

        @pl.when(i >= 2)
        def _():
            wait_parts(i - 2)
            sent_parts(i - 2)

        @pl.when(i >= 5)
        def _():
            done_result(i - 5)

        for u in range(STEP):
            kcopy(u, i).wait()
            if u < STEP - 1:
                vcopy(u, i).wait()

        combine(i - 2)
        for u in range(STEP):
            qp = jnp.dot(pm[...], q_ref[i * STEP + u], preferred_element_type=F32).astype(BF16)
            qq[u, :total, :128] = qp
            qq[u, total:, 128:] = qp
        best = [mx[...]]
        for u in range(STEP):
            high = classes(best[0], heads, jnp.maximum)
            best = [jnp.full((GROUP, 128), -jnp.inf, F32)]
            w = (u + STEP - 1) % STEP
            a = values(high, (u + STEP - 1) % 2, vb[w].at[i % 2 if u else (i + 1) % 2], i, u)
            b = scores(qq[u], u % 2, kb[u].at[i % 2], best)
            for _ in b:
                next(a)
            next(a)

            @pl.when(i < steps - 2)
            def _():
                kcopy(u, i + 2).start()

            @pl.when(i < (steps - 2 if u else steps - 1))
            def _():
                vcopy(w, i + 2 if u else i + 1).start()

        mx[...] = best[0]
        return 0

    lax.fori_loop(0, steps, step, 0)

    send_parts(steps - 1)
    send_result(steps - 3)
    wait_parts(steps - 2)
    vcopy(STEP - 1, steps - 1).wait()
    combine(steps - 2)
    for _ in values(
        classes(mx[...], heads, jnp.maximum), (STEP - 1) % 2, vb[STEP - 1].at[(steps - 1) % 2], steps, 0
    ):
        pass
    send_result(steps - 2)

    b = steps
    for c in range(2):
        d = (2 + c - me + devices) % devices

        @pl.when(d != 0)
        def _():
            o_copy(b, d).start()
            s_copy(b, d).start()

    wait_parts(steps - 1)
    combine(steps - 1)
    send_result(steps - 1)

    @pl.when(chip == 1)
    def _():
        wait_parts(b)
        combine(b)
        send_result(b)

    sent_parts(steps - 2)
    sent_parts(steps - 1)
    for c in range(2):
        d = (2 + c - me + devices) % devices

        @pl.when(d != 0)
        def _():
            o_copy(b, d).wait_send()
            s_copy(b, d).wait_send()

    for i in range(max(steps - 5, 0), steps):
        done_result(i)

    @pl.when(chip == 1)
    def _():
        f_local(b).wait()
        for d in others:
            f_copy(b, d).wait_send()

    for c in range(2):
        d = (me - 2 - c + devices) % devices

        @pl.when(d != 0)
        def _():
            f_copy(b, d).wait_recv()


def solution(mesh):
    devices = mesh.shape["sp"]

    def step(q, k, v):
        n, tokens, heads, d = k.shape
        rows, queries = tokens * heads, q.shape[1]
        total, part, batches = heads * GROUP, queries // 2, n // STEP + 1
        dma = pltpu.SemaphoreType.DMA
        out = pl.pallas_call(
            functools.partial(kernel, n, heads, devices),
            in_specs=[pl.BlockSpec(memory_space=pltpu.VMEM)] + [pl.BlockSpec(memory_space=pl.ANY)] * 2,
            out_specs=pl.BlockSpec(memory_space=pl.ANY),
            out_shape=jax.ShapeDtypeStruct((batches * STEP - STEP + 1, 2, part, d), BF16),
            scratch_shapes=[pltpu.VMEM((2, rows, d), BF16)] * (2 * STEP)
            + [
                pltpu.VMEM((STEP, 2 * total, 2 * d), BF16),
                pltpu.VMEM((2, 2, GROUP, rows // 2), F32),
                pltpu.VMEM((GROUP, 128), F32),
                pltpu.VMEM((total, queries), BF16),
                pltpu.VMEM((queries, total), BF16),
                pltpu.VMEM((total // 2, part), BF16),
                pltpu.VMEM((part, total // 2), BF16),
                pltpu.VMEM((batches, STEP, 2, part, d), BF16),
                pltpu.VMEM((batches, STEP, 8, 128), F32),
                pltpu.VMEM((batches + 2, devices, part, d), BF16),
                pltpu.VMEM((batches + 2, devices, 8, 128), F32),
                pltpu.VMEM((batches + 2, part, d), BF16),
                dma((STEP, 2)),
                dma((STEP, 2)),
                dma((batches, devices)),
                dma((batches, devices)),
                dma((batches, devices)),
                dma((batches, devices)),
                dma((batches, devices)),
                dma((batches, devices)),
                dma((batches,)),
            ],
            compiler_params=pltpu.CompilerParams(
                collective_id=0, has_side_effects=True, vmem_limit_bytes=62 << 20
            ),
            name="attend",
        )(q, k.reshape(n, rows, d), v.reshape(n, rows, d))
        return out[1:].reshape(q.shape)

    return jax.shard_map(
        step,
        mesh=mesh,
        in_specs=(P("dp", None, None), P("dp", "sp", None, None), P("dp", "sp", None, None)),
        out_specs=P("dp", None, None),
        check_vma=False,
    )
```

```python
import functools

import jax
import jax.numpy as jnp
from jax import lax
from jax.experimental import pallas as pl
from jax.experimental.pallas import tpu as pltpu
from jax.sharding import PartitionSpec as P

F32, BF16 = jnp.float32, jnp.bfloat16
LOG2E = 1.4426950408889634
GROUP = 16
STEP = 4
CHUNK = 512


def packed(r, heads, given):
    h, j = r // given, r % given
    return jnp.where(j < 8, 8 * h + j, 8 * heads + (given - 8) * h + j - 8)


def place(heads, given, back=False):
    rows = heads * given
    r = lax.broadcasted_iota(jnp.int32, (rows, rows), 0)
    c = lax.broadcasted_iota(jnp.int32, (rows, rows), 1)
    r, c = (c, r) if back else (r, c)
    return jnp.where(r == packed(c, heads, given), 1.0, 0.0).astype(BF16)


def classes(x, heads, f):
    step = heads
    while step < 128:
        x = f(x, pltpu.roll(x, step, 1))
        step *= 2
    return x


def kernel(n, heads, devices, q_ref, k_hbm, v_hbm, out, *scratch):
    kb, vb = scratch[:STEP], scratch[STEP : 2 * STEP]
    (qq, r_ref, mx, pm, pxt, obuf, sbuf, orecv, srecv, fbuf) = scratch[2 * STEP : 2 * STEP + 10]
    (ksem, vsem, o_send, s_send, o_recv, s_recv, f_send, f_recv, f_own) = scratch[2 * STEP + 10 :]
    rows = k_hbm.shape[1]
    half = rows // 2
    total = q_ref.shape[1]
    given = total // heads
    first = heads * 8
    pairs = heads // 2
    part = q_ref.shape[1] // 2
    scale = q_ref.shape[2] ** -0.5 * LOG2E
    steps = n // STEP
    me = lax.axis_index("sp")
    chip, core = me // 2, me % 2
    mine = (chip + STEP - 1) % STEP

    lane = lax.broadcasted_iota(jnp.int32, (GROUP, 128), 1)
    row = lax.broadcasted_iota(jnp.int32, (GROUP, 128), 0)
    kind = lane % heads
    lane8 = lane[:8]
    masks = [kind[:8] == h for h in range(heads)]
    twos = [kind[:8] // 2 == p for p in range(pairs)]
    keep = [kind == 2 * g + row // 8 for g in range(pairs)]
    keep += [kind == 4 * g + row // 4 for g in range(pairs // 2)]
    keep = [m.astype(F32).astype(BF16) for m in keep]

    def kcopy(u, i):
        return pltpu.make_async_copy(k_hbm.at[jnp.minimum(i * STEP + u, n - 1)], kb[u].at[i % 2], ksem.at[u, i % 2])

    def vcopy(u, i):
        return pltpu.make_async_copy(v_hbm.at[jnp.minimum(i * STEP + u, n - 1)], vb[u].at[i % 2], vsem.at[u, i % 2])

    def o_copy(b, d):
        peer = (me + d) % devices
        turn = (peer // 2 + STEP - 1) % STEP
        return pltpu.make_async_remote_copy(
            obuf.at[b, turn, peer % 2], orecv.at[b + 2, d], o_send.at[b, d], o_recv.at[b, d], device_id={"sp": peer}
        )

    def s_copy(b, d):
        peer = (me + d) % devices
        turn = (peer // 2 + STEP - 1) % STEP
        return pltpu.make_async_remote_copy(
            sbuf.at[b, turn], srecv.at[b + 2, d], s_send.at[b, d], s_recv.at[b, d], device_id={"sp": peer}
        )

    def f_copy(b, d):
        peer = (me + d) % devices
        return pltpu.make_async_remote_copy(
            fbuf.at[b + 2], out.at[jnp.minimum(b * STEP + mine, n), core], f_send.at[b, d], f_recv.at[b, d], device_id={"sp": peer}
        )

    def f_local(b):
        return pltpu.make_async_copy(fbuf.at[b + 2], out.at[jnp.minimum(b * STEP + mine, n), core], f_own.at[b])

    others = range(1, devices)

    def send_parts(b):
        for d in others:
            o_copy(b, d).start()
            s_copy(b, d).start()

    def wait_parts(b):
        for d in others:
            o_copy(b, d).wait_recv()
            s_copy(b, d).wait_recv()

    def sent_parts(b):
        for d in others:
            o_copy(b, d).wait_send()
            s_copy(b, d).wait_send()

    def send_result(b):
        f_local(b).start()
        for d in others:
            f_copy(b, d).start()

    def done_result(b):
        f_local(b).wait()
        for d in others:
            f_copy(b, d).wait_send()
            f_copy(b, d).wait_recv()

    def combine(b):
        own = jnp.maximum(b, 0)
        stats = [sbuf[own, mine]] + [srecv[b + 2, d] for d in others]
        parts = [obuf[own, mine, core]] + [orecv[b + 2, d] for d in others]
        high = functools.reduce(jnp.maximum, stats)
        scales = [jnp.exp2((s - high) * scale) for s in stats]
        below = functools.reduce(jnp.add, [a * pltpu.roll(s, 128 - heads, 1) for a, s in zip(scales, stats)])
        inverse = 1.0 / below
        sums = jnp.zeros((part, 128), F32)
        for x, a in zip(parts, scales):
            w = a * inverse
            w = jnp.where(core == 0, w, pltpu.roll(w, 128 - heads // 2, 1))
            w = [jnp.broadcast_to(w[:, e : e + 1], (8, 128)) for e in (*range(pairs), *range(64, 64 + pairs))]
            w = w[:pairs] + [jnp.where(row[:8] < 4, w[pairs + p], w[pairs + p + 1]) for p in range(0, pairs, 2)]
            sums = sums + x.astype(F32) * jnp.concatenate(w, 0)
        fbuf[b + 2] = jnp.dot(pxt[...], sums.astype(BF16), preferred_element_type=F32).astype(BF16)

    def values(high, source, v, b, u):
        base = high * scale
        seen = jnp.zeros((2 * total, 256), F32)
        sums = jnp.zeros((GROUP, 128), F32)
        t = CHUNK // 128 if half >= CHUNK else half // 128
        size = t * 128
        for c in range(half // size):
            parts = []
            for side in range(2):
                for x in range(t):
                    p = jnp.exp2(r_ref[source, side, :, pl.ds(c * size + x * 128, 128)] * scale - base)
                    sums = sums + p
                    parts.append([jnp.concatenate([y, y], 0).astype(BF16) for y in (p[:8], p[8:])])
            spread = jnp.concatenate(
                [
                    jnp.concatenate([parts[side * t + x][g // pairs] * m for x in range(t)], 1)
                    for side in range(2)
                    for g, m in enumerate(keep)
                ],
                0,
            )
            vv = jnp.concatenate([v[pl.ds(c * size, size)], v[pl.ds(half + c * size, size)]], 1)
            seen = seen + jnp.dot(spread, vv, preferred_element_type=F32)
            yield
        sums = classes(sums, heads, jnp.add)
        o = (seen[:total, :128] + seen[total:, 128:]).astype(BF16)
        for c in range(2):
            obuf[b, u, c, : first // 2] = o[c * first // 2 : (c + 1) * first // 2]
            obuf[b, u, c, first // 2 :] = o[first + c * (part - first // 2) : first + (c + 1) * (part - first // 2)]
        even = lane8 // heads % 2 == 0
        low = jnp.where(even, high[:8], sums[:8])
        high = jnp.where(even, high[8:], sums[8:])
        sbuf[b, u] = jnp.where(lane8 < 64, low, high)
        yield

    def scores(query, target, k, best):
        t = CHUNK // 128 if half >= CHUNK else half // 128
        size = t * 128
        for c in range(half // size):
            kk = jnp.concatenate([k[pl.ds(c * size, size)], k[pl.ds(half + c * size, size)]], 1)
            s = lax.dot_general(query, kk, (((1,), (1,)), ((), ())), preferred_element_type=F32)
            for side in range(2):
                for x in range(t):
                    cols = slice(x * 128, (x + 1) * 128)
                    block = [s[side * total + e : side * total + e + 8, cols] for e in range(0, total, 8)]
                    r = [block[0], block[heads]]
                    for h in range(1, heads):
                        r[0] = jnp.where(masks[h], block[h], r[0])
                    for p in range(1, pairs):
                        r[1] = jnp.where(twos[p], block[heads + p], r[1])
                    r = jnp.concatenate(r, 0)
                    r_ref[target, side, :, pl.ds(c * size + x * 128, 128)] = r
                    best[0] = jnp.maximum(best[0], r)
            yield

    for i in range(2):
        for u in range(STEP):
            kcopy(u, i).start()
            if (i, u) != (1, STEP - 1):
                vcopy(u, i).start()

    barrier = pltpu.get_barrier_semaphore()
    for d in others:
        pl.semaphore_signal(barrier, inc=1, device_id={"sp": (me + d) % devices})
    pl.semaphore_wait(barrier, devices - 1)

    pm[...] = place(heads, given)
    pxt[...] = place(heads // 2, given, back=True)
    qq[...] = jnp.zeros_like(qq)
    r_ref[...] = jnp.zeros_like(r_ref)
    mx[...] = jnp.zeros_like(mx)

    def step(i, _):
        for u in range(STEP):
            kcopy(u, i).wait()
            if u < STEP - 1:
                vcopy(u, i).wait()

        @pl.when(i >= 1)
        def _():
            vcopy(STEP - 1, i - 1).wait()
            send_parts(i - 1)

        @pl.when(i >= 3)
        def _():
            send_result(i - 3)

        @pl.when(i >= 2)
        def _():
            wait_parts(i - 2)
            sent_parts(i - 2)

        @pl.when(i >= 5)
        def _():
            done_result(i - 5)

        combine(i - 2)
        for u in range(STEP):
            qp = jnp.dot(pm[...], q_ref[i * STEP + u], preferred_element_type=F32).astype(BF16)
            qq[u, :total, :128] = qp
            qq[u, total:, 128:] = qp
        best = [mx[...]]
        for u in range(STEP):
            high = classes(best[0], heads, jnp.maximum)
            best = [jnp.full((GROUP, 128), -jnp.inf, F32)]
            w = (u + STEP - 1) % STEP
            a = values(high, (u + STEP - 1) % 2, vb[w].at[i % 2 if u else (i + 1) % 2], i, u)
            b = scores(qq[u], u % 2, kb[u].at[i % 2], best)
            for _ in b:
                next(a)
            next(a)

            @pl.when(i < steps - 2)
            def _():
                kcopy(u, i + 2).start()

            @pl.when(i < (steps - 2 if u else steps - 1))
            def _():
                vcopy(w, i + 2 if u else i + 1).start()

        mx[...] = best[0]
        return 0

    lax.fori_loop(0, steps, step, 0)

    send_parts(steps - 1)
    send_result(steps - 3)
    wait_parts(steps - 2)
    vcopy(STEP - 1, steps - 1).wait()
    combine(steps - 2)
    for _ in values(
        classes(mx[...], heads, jnp.maximum), (STEP - 1) % 2, vb[STEP - 1].at[(steps - 1) % 2], steps, 0
    ):
        pass
    send_result(steps - 2)

    b = steps
    for c in range(2):
        d = (2 + c - me + devices) % devices

        @pl.when(d != 0)
        def _():
            o_copy(b, d).start()
            s_copy(b, d).start()

    wait_parts(steps - 1)
    combine(steps - 1)
    send_result(steps - 1)

    @pl.when(chip == 1)
    def _():
        wait_parts(b)
        combine(b)
        send_result(b)

    sent_parts(steps - 2)
    sent_parts(steps - 1)
    for c in range(2):
        d = (2 + c - me + devices) % devices

        @pl.when(d != 0)
        def _():
            o_copy(b, d).wait_send()
            s_copy(b, d).wait_send()

    for i in range(max(steps - 5, 0), steps):
        done_result(i)

    @pl.when(chip == 1)
    def _():
        f_local(b).wait()
        for d in others:
            f_copy(b, d).wait_send()

    for c in range(2):
        d = (me - 2 - c + devices) % devices

        @pl.when(d != 0)
        def _():
            f_copy(b, d).wait_recv()


def solution(mesh):
    devices = mesh.shape["sp"]

    def step(q, k, v):
        n, tokens, heads, d = k.shape
        rows, queries = tokens * heads, q.shape[1]
        part, batches = queries // 2, n // STEP + 1
        dma = pltpu.SemaphoreType.DMA
        out = pl.pallas_call(
            functools.partial(kernel, n, heads, devices),
            in_specs=[pl.BlockSpec(memory_space=pltpu.VMEM)] + [pl.BlockSpec(memory_space=pl.ANY)] * 2,
            out_specs=pl.BlockSpec(memory_space=pl.ANY),
            out_shape=jax.ShapeDtypeStruct((batches * STEP - STEP + 1, 2, part, d), BF16),
            scratch_shapes=[pltpu.VMEM((2, rows, d), BF16)] * (2 * STEP)
            + [
                pltpu.VMEM((STEP, 2 * queries, 2 * d), BF16),
                pltpu.VMEM((2, 2, GROUP, rows // 2), F32),
                pltpu.VMEM((GROUP, 128), F32),
                pltpu.VMEM((queries, queries), BF16),
                pltpu.VMEM((part, part), BF16),
                pltpu.VMEM((batches, STEP, 2, part, d), BF16),
                pltpu.VMEM((batches, STEP, 8, 128), F32),
                pltpu.VMEM((batches + 2, devices, part, d), BF16),
                pltpu.VMEM((batches + 2, devices, 8, 128), F32),
                pltpu.VMEM((batches + 2, part, d), BF16),
                dma((STEP, 2)),
                dma((STEP, 2)),
                dma((batches, devices)),
                dma((batches, devices)),
                dma((batches, devices)),
                dma((batches, devices)),
                dma((batches, devices)),
                dma((batches, devices)),
                dma((batches,)),
            ],
            compiler_params=pltpu.CompilerParams(
                collective_id=0, has_side_effects=True, vmem_limit_bytes=62 << 20
            ),
            name="attend",
        )(q, k.reshape(n, rows, d), v.reshape(n, rows, d))
        return out[1:].reshape(q.shape)

    return jax.shard_map(
        step,
        mesh=mesh,
        in_specs=(P("dp", None, None), P("dp", "sp", None, None), P("dp", "sp", None, None)),
        out_specs=P("dp", None, None),
        check_vma=False,
    )
```

```python
import functools

import jax
import jax.numpy as jnp
from jax import lax
from jax.experimental import pallas as pl
from jax.experimental.pallas import tpu as pltpu
from jax.sharding import PartitionSpec as P

F32, BF16 = jnp.float32, jnp.bfloat16
LOG2E = 1.4426950408889634
GROUP = 16
STEP = 4
CHUNK = 256


def packed(r, heads, given):
    h, j = r // given, r % given
    return jnp.where(j < 8, 8 * h + j, 8 * heads + (given - 8) * h + j - 8)


def place(heads, given, back=False):
    rows = heads * given
    r = lax.broadcasted_iota(jnp.int32, (rows, rows), 0)
    c = lax.broadcasted_iota(jnp.int32, (rows, rows), 1)
    r, c = (c, r) if back else (r, c)
    return jnp.where(r == packed(c, heads, given), 1.0, 0.0).astype(BF16)


def classes(x, heads, f):
    step = heads
    while step < 128:
        x = f(x, pltpu.roll(x, step, 1))
        step *= 2
    return x


def kernel(n, heads, devices, q_ref, k_hbm, v_hbm, out, *scratch):
    kb, vb = scratch[:STEP], scratch[STEP : 2 * STEP]
    (qq, r_ref, mx, pm, pxt, obuf, sbuf, orecv, srecv, fbuf) = scratch[2 * STEP : 2 * STEP + 10]
    (ksem, vsem, o_send, s_send, o_recv, s_recv, f_send, f_recv, f_own) = scratch[2 * STEP + 10 :]
    rows = k_hbm.shape[1]
    half = rows // 2
    total = q_ref.shape[1]
    given = total // heads
    first = heads * 8
    pairs = heads // 2
    part = q_ref.shape[1] // 2
    scale = q_ref.shape[2] ** -0.5 * LOG2E
    steps = n // STEP
    me = lax.axis_index("sp")
    chip, core = me // 2, me % 2
    mine = (chip + 2) % STEP

    lane = lax.broadcasted_iota(jnp.int32, (GROUP, 128), 1)
    row = lax.broadcasted_iota(jnp.int32, (GROUP, 128), 0)
    kind = lane % heads
    lane8 = lane[:8]
    masks = [kind[:8] == h for h in range(heads)]
    twos = [kind[:8] // 2 == p for p in range(pairs)]
    keep = [kind == 2 * g + row // 8 for g in range(pairs)]
    keep += [kind == 4 * g + row // 4 for g in range(pairs // 2)]
    keep = [m.astype(F32).astype(BF16) for m in keep]

    def kcopy(u, i):
        return pltpu.make_async_copy(k_hbm.at[jnp.minimum(i * STEP + u, n - 1)], kb[u].at[i % 2], ksem.at[u, i % 2])

    def vcopy(u, i):
        return pltpu.make_async_copy(v_hbm.at[jnp.minimum(i * STEP + u, n - 1)], vb[u].at[i % 2], vsem.at[u, i % 2])

    def o_copy(b, d):
        peer = (me + d) % devices
        turn = (peer // 2 + 2) % STEP
        return pltpu.make_async_remote_copy(
            obuf.at[b, turn, peer % 2], orecv.at[b + 2, d], o_send.at[b, d], o_recv.at[b, d], device_id={"sp": peer}
        )

    def s_copy(b, d):
        peer = (me + d) % devices
        turn = (peer // 2 + 2) % STEP
        return pltpu.make_async_remote_copy(
            sbuf.at[b, turn], srecv.at[b + 2, d], s_send.at[b, d], s_recv.at[b, d], device_id={"sp": peer}
        )

    def f_copy(b, d):
        peer = (me + d) % devices
        return pltpu.make_async_remote_copy(
            fbuf.at[b + 2], out.at[b * STEP + mine, core], f_send.at[b, d], f_recv.at[b, d], device_id={"sp": peer}
        )

    def f_local(b):
        return pltpu.make_async_copy(fbuf.at[b + 2], out.at[b * STEP + mine, core], f_own.at[b])

    others = range(1, devices)

    def send_parts(b):
        for d in others:
            o_copy(b, d).start()
            s_copy(b, d).start()

    def wait_parts(b):
        for d in others:
            o_copy(b, d).wait_recv()
            s_copy(b, d).wait_recv()

    def sent_parts(b):
        for d in others:
            o_copy(b, d).wait_send()
            s_copy(b, d).wait_send()

    def send_result(b):
        f_local(b).start()
        for d in others:
            f_copy(b, d).start()

    def done_result(b):
        f_local(b).wait()
        for d in others:
            f_copy(b, d).wait_send()
            f_copy(b, d).wait_recv()

    def combine(b):
        own = jnp.maximum(b, 0)
        stats = [sbuf[own, mine]] + [srecv[b + 2, d] for d in others]
        parts = [obuf[own, mine, core]] + [orecv[b + 2, d] for d in others]
        high = functools.reduce(jnp.maximum, stats)
        scales = [jnp.exp2((s - high) * scale) for s in stats]
        below = functools.reduce(jnp.add, [a * pltpu.roll(s, 128 - heads, 1) for a, s in zip(scales, stats)])
        inverse = 1.0 / below
        sums = jnp.zeros((part, 128), F32)
        for x, a in zip(parts, scales):
            w = a * inverse
            w = jnp.where(core == 0, w, pltpu.roll(w, 128 - heads // 2, 1))
            w = [jnp.broadcast_to(w[:, e : e + 1], (8, 128)) for e in (*range(pairs), *range(64, 64 + pairs))]
            w = w[:pairs] + [jnp.where(row[:8] < 4, w[pairs + p], w[pairs + p + 1]) for p in range(0, pairs, 2)]
            sums = sums + x.astype(F32) * jnp.concatenate(w, 0)
        fbuf[b + 2] = jnp.dot(pxt[...], sums.astype(BF16), preferred_element_type=F32).astype(BF16)

    def values(high, source, v, b, u):
        base = high * scale
        seen = jnp.zeros((2 * total, 256), F32)
        sums = jnp.zeros((GROUP, 128), F32)
        t = CHUNK // 128 if half >= CHUNK else half // 128
        size = t * 128
        for c in range(half // size):
            parts = []
            for side in range(2):
                for x in range(t):
                    p = jnp.exp2(r_ref[source, side, :, pl.ds(c * size + x * 128, 128)] * scale - base)
                    sums = sums + p
                    parts.append([jnp.concatenate([y, y], 0).astype(BF16) for y in (p[:8], p[8:])])
            spread = jnp.concatenate(
                [
                    jnp.concatenate([parts[side * t + x][g // pairs] * m for x in range(t)], 1)
                    for side in range(2)
                    for g, m in enumerate(keep)
                ],
                0,
            )
            vv = jnp.concatenate([v[pl.ds(c * size, size)], v[pl.ds(half + c * size, size)]], 1)
            seen = seen + jnp.dot(spread, vv, preferred_element_type=F32)
            yield
        sums = classes(sums, heads, jnp.add)
        o = (seen[:total, :128] + seen[total:, 128:]).astype(BF16)
        for c in range(2):
            obuf[b, u, c, : first // 2] = o[c * first // 2 : (c + 1) * first // 2]
            obuf[b, u, c, first // 2 :] = o[first + c * (part - first // 2) : first + (c + 1) * (part - first // 2)]
        even = lane8 // heads % 2 == 0
        low = jnp.where(even, high[:8], sums[:8])
        high = jnp.where(even, high[8:], sums[8:])
        sbuf[b, u] = jnp.where(lane8 < 64, low, high)
        yield

    def scores(query, target, k, best):
        t = CHUNK // 128 if half >= CHUNK else half // 128
        size = t * 128
        for c in range(half // size):
            kk = jnp.concatenate([k[pl.ds(c * size, size)], k[pl.ds(half + c * size, size)]], 1)
            s = lax.dot_general(query, kk, (((1,), (1,)), ((), ())), preferred_element_type=F32)
            for side in range(2):
                for x in range(t):
                    cols = slice(x * 128, (x + 1) * 128)
                    block = [s[side * total + e : side * total + e + 8, cols] for e in range(0, total, 8)]
                    r = [block[0], block[heads]]
                    for h in range(1, heads):
                        r[0] = jnp.where(masks[h], block[h], r[0])
                    for p in range(1, pairs):
                        r[1] = jnp.where(twos[p], block[heads + p], r[1])
                    r = jnp.concatenate(r, 0)
                    r_ref[target, side, :, pl.ds(c * size + x * 128, 128)] = r
                    best[0] = jnp.maximum(best[0], r)
            yield

    kcopy(0, 0).start()
    for x in range(2 * STEP):
        if x < 2 * STEP - 1:
            kcopy((x + 1) % STEP, (x + 1) // STEP).start()
        vcopy(x % STEP, x // STEP).start()

    barrier = pltpu.get_barrier_semaphore()
    for d in others:
        pl.semaphore_signal(barrier, inc=1, device_id={"sp": (me + d) % devices})
    pl.semaphore_wait(barrier, devices - 1)

    pm[...] = place(heads, given)
    pxt[...] = place(heads // 2, given, back=True)
    qq[...] = jnp.zeros_like(qq)

    def query(slot, s):
        qp = jnp.dot(pm[...], q_ref[jnp.minimum(s, n - 1)], preferred_element_type=F32).astype(BF16)
        qq[slot, :total, :128] = qp
        qq[slot, total:, 128:] = qp

    lowest = jnp.full((GROUP, 128), -jnp.inf, F32)
    query(0, 0)
    kcopy(0, 0).wait()
    best = [lowest]
    for _ in scores(qq[0], 0, kb[0].at[0], best):
        pass
    mx[...] = best[0]
    kcopy(0, 2).start()

    def step(i, _):
        for u in range(STEP):
            vcopy(u, i).wait()
            if u:
                kcopy(u, i).wait()

        @pl.when(i < steps - 1)
        def _():
            kcopy(0, i + 1).wait()

        @pl.when(i >= 2)
        def _():
            wait_parts(i - 2)
            sent_parts(i - 2)

        @pl.when(i >= 5)
        def _():
            done_result(i - 5)

        combine(i - 2)
        for u in range(STEP):
            query(u, i * STEP + u + 1)
        best = [mx[...]]
        for u in range(STEP):
            high = classes(best[0], heads, jnp.maximum)
            best = [lowest]
            w, turn = (u + 1) % STEP, (u + 1) // STEP
            a = values(high, u % 2, vb[u].at[i % 2], i, u)
            b = scores(qq[u], w % 2, kb[w].at[(i + turn) % 2], best)
            for _ in b:
                next(a)
            next(a)

            @pl.when(i + turn < steps - 2)
            def _():
                kcopy(w, i + turn + 2).start()

            @pl.when(i < steps - 2)
            def _():
                vcopy(u, i + 2).start()

        mx[...] = best[0]
        send_parts(i)

        @pl.when(i >= 2)
        def _():
            send_result(i - 2)

        return 0

    lax.fori_loop(0, steps, step, 0)

    for b in range(steps - 2, steps):
        wait_parts(b)
        combine(b)
        send_result(b)
    for b in range(steps - 2, steps):
        sent_parts(b)
    for b in range(max(steps - 5, 0), steps):
        done_result(b)


def solution(mesh):
    devices = mesh.shape["sp"]

    def step(q, k, v):
        n, tokens, heads, d = k.shape
        rows, queries = tokens * heads, q.shape[1]
        part, batches = queries // 2, n // STEP
        dma = pltpu.SemaphoreType.DMA
        out = pl.pallas_call(
            functools.partial(kernel, n, heads, devices),
            in_specs=[pl.BlockSpec(memory_space=pltpu.VMEM)] + [pl.BlockSpec(memory_space=pl.ANY)] * 2,
            out_specs=pl.BlockSpec(memory_space=pl.ANY),
            out_shape=jax.ShapeDtypeStruct((n, 2, part, d), BF16),
            scratch_shapes=[pltpu.VMEM((2, rows, d), BF16)] * (2 * STEP)
            + [
                pltpu.VMEM((STEP, 2 * queries, 2 * d), BF16),
                pltpu.VMEM((2, 2, GROUP, rows // 2), F32),
                pltpu.VMEM((GROUP, 128), F32),
                pltpu.VMEM((queries, queries), BF16),
                pltpu.VMEM((part, part), BF16),
                pltpu.VMEM((batches, STEP, 2, part, d), BF16),
                pltpu.VMEM((batches, STEP, 8, 128), F32),
                pltpu.VMEM((batches + 2, devices, part, d), BF16),
                pltpu.VMEM((batches + 2, devices, 8, 128), F32),
                pltpu.VMEM((batches + 2, part, d), BF16),
                dma((STEP, 2)),
                dma((STEP, 2)),
                dma((batches, devices)),
                dma((batches, devices)),
                dma((batches, devices)),
                dma((batches, devices)),
                dma((batches, devices)),
                dma((batches, devices)),
                dma((batches,)),
            ],
            compiler_params=pltpu.CompilerParams(
                collective_id=0, has_side_effects=True, vmem_limit_bytes=62 << 20
            ),
            name="attend",
        )(q, k.reshape(n, rows, d), v.reshape(n, rows, d))
        return out.reshape(q.shape)

    return jax.shard_map(
        step,
        mesh=mesh,
        in_specs=(P("dp", None, None), P("dp", "sp", None, None), P("dp", "sp", None, None)),
        out_specs=P("dp", None, None),
        check_vma=False,
    )
```

```python
import functools

import jax
import jax.numpy as jnp
from jax import lax
from jax.experimental import pallas as pl
from jax.experimental.pallas import tpu as pltpu
from jax.sharding import PartitionSpec as P

F32, BF16 = jnp.float32, jnp.bfloat16
LOG2E = 1.4426950408889634
GROUP = 16
STEP = 4
CHUNK = 256


def packed(r, heads, given):
    h, j = r // given, r % given
    return jnp.where(j < 8, 8 * h + j, 8 * heads + (given - 8) * h + j - 8)


def place(heads, given, back=False):
    rows = heads * given
    r = lax.broadcasted_iota(jnp.int32, (rows, rows), 0)
    c = lax.broadcasted_iota(jnp.int32, (rows, rows), 1)
    r, c = (c, r) if back else (r, c)
    return jnp.where(r == packed(c, heads, given), 1.0, 0.0).astype(BF16)


def classes(x, heads, f):
    step = heads
    while step < 128:
        x = f(x, pltpu.roll(x, step, 1))
        step *= 2
    return x


def kernel(n, heads, devices, q_ref, k_hbm, v_hbm, out, *scratch):
    kb, vb = scratch[:STEP], scratch[STEP : 2 * STEP]
    (qq, r_ref, mx, pm, pxt, obuf, sbuf, orecv, srecv, fbuf) = scratch[2 * STEP : 2 * STEP + 10]
    (ksem, vsem, o_send, s_send, o_recv, s_recv, f_send, f_recv, f_own) = scratch[2 * STEP + 10 :]
    rows = k_hbm.shape[1]
    half = rows // 2
    total = q_ref.shape[1]
    given = total // heads
    first = heads * 8
    pairs = heads // 2
    part = q_ref.shape[1] // 2
    scale = q_ref.shape[2] ** -0.5 * LOG2E
    steps = n // STEP
    me = lax.axis_index("sp")
    chip, core = me // 2, me % 2
    mine = (chip + 2) % STEP

    lane = lax.broadcasted_iota(jnp.int32, (GROUP, 128), 1)
    row = lax.broadcasted_iota(jnp.int32, (GROUP, 128), 0)
    kind = lane % heads
    lane8 = lane[:8]
    masks = [kind[:8] == h for h in range(heads)]
    twos = [kind[:8] // 2 == p for p in range(pairs)]
    keep = [kind == 2 * g + row // 8 for g in range(pairs)]
    keep += [kind == 4 * g + row // 4 for g in range(pairs // 2)]
    keep = [m.astype(F32).astype(BF16) for m in keep]

    def kcopy(u, i):
        return pltpu.make_async_copy(k_hbm.at[jnp.minimum(i * STEP + u, n - 1)], kb[u].at[i % 2], ksem.at[u, i % 2])

    def vcopy(u, i):
        return pltpu.make_async_copy(v_hbm.at[jnp.minimum(i * STEP + u, n - 1)], vb[u].at[i % 2], vsem.at[u, i % 2])

    def o_copy(b, d):
        peer = (me + d) % devices
        turn = (peer // 2 + 2) % STEP
        return pltpu.make_async_remote_copy(
            obuf.at[b, turn, peer % 2], orecv.at[b + 2, d], o_send.at[b, d], o_recv.at[b, d], device_id={"sp": peer}
        )

    def s_copy(b, d):
        peer = (me + d) % devices
        turn = (peer // 2 + 2) % STEP
        return pltpu.make_async_remote_copy(
            sbuf.at[b, turn], srecv.at[b + 2, d], s_send.at[b, d], s_recv.at[b, d], device_id={"sp": peer}
        )

    def f_copy(b, d):
        peer = (me + d) % devices
        return pltpu.make_async_remote_copy(
            fbuf.at[b + 2], out.at[b * STEP + mine, core], f_send.at[b, d], f_recv.at[b, d], device_id={"sp": peer}
        )

    def f_local(b):
        return pltpu.make_async_copy(fbuf.at[b + 2], out.at[b * STEP + mine, core], f_own.at[b])

    others = range(1, devices)

    def send_parts(b):
        for d in others:
            o_copy(b, d).start()
            s_copy(b, d).start()

    def send_turns(b, turns):
        for d in others:
            turn = ((me + d) % devices // 2 + 2) % STEP

            @pl.when((turn >= turns.start) & (turn < turns.stop))
            def _():
                o_copy(b, d).start()
                s_copy(b, d).start()

    def wait_parts(b):
        for d in others:
            o_copy(b, d).wait_recv()
            s_copy(b, d).wait_recv()

    def sent_parts(b):
        for d in others:
            o_copy(b, d).wait_send()
            s_copy(b, d).wait_send()

    def send_result(b):
        f_local(b).start()
        for d in others:
            f_copy(b, d).start()

    def done_result(b):
        f_local(b).wait()
        for d in others:
            f_copy(b, d).wait_send()
            f_copy(b, d).wait_recv()

    def combine(b):
        own = jnp.maximum(b, 0)
        stats = [sbuf[own, mine]] + [srecv[b + 2, d] for d in others]
        parts = [obuf[own, mine, core]] + [orecv[b + 2, d] for d in others]
        high = functools.reduce(jnp.maximum, stats)
        scales = [jnp.exp2((s - high) * scale) for s in stats]
        below = functools.reduce(jnp.add, [a * pltpu.roll(s, 128 - heads, 1) for a, s in zip(scales, stats)])
        inverse = 1.0 / below
        sums = jnp.zeros((part, 128), F32)
        for x, a in zip(parts, scales):
            w = a * inverse
            w = jnp.where(core == 0, w, pltpu.roll(w, 128 - heads // 2, 1))
            w = [jnp.broadcast_to(w[:, e : e + 1], (8, 128)) for e in (*range(pairs), *range(64, 64 + pairs))]
            w = w[:pairs] + [jnp.where(row[:8] < 4, w[pairs + p], w[pairs + p + 1]) for p in range(0, pairs, 2)]
            sums = sums + x.astype(F32) * jnp.concatenate(w, 0)
        fbuf[b + 2] = jnp.dot(pxt[...], sums.astype(BF16), preferred_element_type=F32).astype(BF16)

    def values(high, source, v, b, u):
        base = high * scale
        seen = jnp.zeros((2 * total, 256), F32)
        sums = jnp.zeros((GROUP, 128), F32)
        t = CHUNK // 128 if half >= CHUNK else half // 128
        size = t * 128
        for c in range(half // size):
            parts = []
            for side in range(2):
                for x in range(t):
                    p = jnp.exp2(r_ref[source, side, :, pl.ds(c * size + x * 128, 128)] * scale - base)
                    sums = sums + p
                    parts.append([jnp.concatenate([y, y], 0).astype(BF16) for y in (p[:8], p[8:])])
            spread = jnp.concatenate(
                [
                    jnp.concatenate([parts[side * t + x][g // pairs] * m for x in range(t)], 1)
                    for side in range(2)
                    for g, m in enumerate(keep)
                ],
                0,
            )
            vv = jnp.concatenate([v[pl.ds(c * size, size)], v[pl.ds(half + c * size, size)]], 1)
            seen = seen + jnp.dot(spread, vv, preferred_element_type=F32)
            yield
        sums = classes(sums, heads, jnp.add)
        o = (seen[:total, :128] + seen[total:, 128:]).astype(BF16)
        for c in range(2):
            obuf[b, u, c, : first // 2] = o[c * first // 2 : (c + 1) * first // 2]
            obuf[b, u, c, first // 2 :] = o[first + c * (part - first // 2) : first + (c + 1) * (part - first // 2)]
        even = lane8 // heads % 2 == 0
        low = jnp.where(even, high[:8], sums[:8])
        high = jnp.where(even, high[8:], sums[8:])
        sbuf[b, u] = jnp.where(lane8 < 64, low, high)
        yield

    def scores(query, target, k, best):
        t = CHUNK // 128 if half >= CHUNK else half // 128
        size = t * 128
        for c in range(half // size):
            kk = jnp.concatenate([k[pl.ds(c * size, size)], k[pl.ds(half + c * size, size)]], 1)
            s = lax.dot_general(query, kk, (((1,), (1,)), ((), ())), preferred_element_type=F32)
            for side in range(2):
                for x in range(t):
                    cols = slice(x * 128, (x + 1) * 128)
                    block = [s[side * total + e : side * total + e + 8, cols] for e in range(0, total, 8)]
                    r = [block[0], block[heads]]
                    for h in range(1, heads):
                        r[0] = jnp.where(masks[h], block[h], r[0])
                    for p in range(1, pairs):
                        r[1] = jnp.where(twos[p], block[heads + p], r[1])
                    r = jnp.concatenate(r, 0)
                    r_ref[target, side, :, pl.ds(c * size + x * 128, 128)] = r
                    best[0] = jnp.maximum(best[0], r)
            yield

    kcopy(0, 0).start()
    for x in range(2 * STEP):
        if x < 2 * STEP - 1:
            kcopy((x + 1) % STEP, (x + 1) // STEP).start()
        vcopy(x % STEP, x // STEP).start()

    barrier = pltpu.get_barrier_semaphore()
    for d in others:
        pl.semaphore_signal(barrier, inc=1, device_id={"sp": (me + d) % devices})
    pl.semaphore_wait(barrier, devices - 1)

    pm[...] = place(heads, given)
    pxt[...] = place(heads // 2, given, back=True)
    qq[...] = jnp.zeros_like(qq)

    def query(slot, s):
        qp = jnp.dot(pm[...], q_ref[jnp.minimum(s, n - 1)], preferred_element_type=F32).astype(BF16)
        qq[slot, :total, :128] = qp
        qq[slot, total:, 128:] = qp

    lowest = jnp.full((GROUP, 128), -jnp.inf, F32)
    query(0, 0)
    kcopy(0, 0).wait()
    best = [lowest]
    for _ in scores(qq[0], 0, kb[0].at[0], best):
        pass
    mx[...] = best[0]
    kcopy(0, 2).start()

    def part_of(i, turns, last=False):
        for u in turns:
            query(u, i * STEP + u + 1)
        best = [mx[...]]
        for u in turns:
            high = classes(best[0], heads, jnp.maximum)
            best = [lowest]
            w, turn = (u + 1) % STEP, (u + 1) // STEP
            a = values(high, u % 2, vb[u].at[i % 2], i, u)
            if not (last and turn):
                for _ in scores(qq[u], w % 2, kb[w].at[(i + turn) % 2], best):
                    next(a)
            for _ in a:
                pass
            if last:
                continue

            @pl.when(i + turn < steps - 2)
            def _():
                kcopy(w, i + turn + 2).start()

            @pl.when(i < steps - 2)
            def _():
                vcopy(u, i + 2).start()

        mx[...] = best[0]

    def step(i, _):
        for u in range(STEP):
            vcopy(u, i).wait()
            if u:
                kcopy(u, i).wait()

        kcopy(0, i + 1).wait()

        @pl.when(i >= 2)
        def _():
            wait_parts(i - 2)
            sent_parts(i - 2)

        @pl.when(i >= 5)
        def _():
            done_result(i - 5)

        combine(i - 2)
        part_of(i, range(STEP))
        send_parts(i)

        @pl.when(i >= 2)
        def _():
            send_result(i - 2)

        return 0

    lax.fori_loop(0, steps - 1, step, 0)

    b = steps - 1
    for u in range(STEP):
        vcopy(u, b).wait()
        if u:
            kcopy(u, b).wait()
    wait_parts(b - 2)
    sent_parts(b - 2)
    combine(b - 2)
    part_of(b, range(STEP // 2), last=True)
    send_turns(b, range(STEP // 2))
    send_result(b - 2)
    wait_parts(b - 1)
    combine(b - 1)
    part_of(b, range(STEP // 2, STEP), last=True)
    send_turns(b, range(STEP // 2, STEP))
    send_result(b - 1)

    wait_parts(b)
    combine(b)
    send_result(b)
    for b in range(steps - 2, steps):
        sent_parts(b)
    for b in range(max(steps - 6, 0), steps):
        done_result(b)


def solution(mesh):
    devices = mesh.shape["sp"]

    def step(q, k, v):
        n, tokens, heads, d = k.shape
        rows, queries = tokens * heads, q.shape[1]
        part, batches = queries // 2, n // STEP
        dma = pltpu.SemaphoreType.DMA
        out = pl.pallas_call(
            functools.partial(kernel, n, heads, devices),
            in_specs=[pl.BlockSpec(memory_space=pltpu.VMEM)] + [pl.BlockSpec(memory_space=pl.ANY)] * 2,
            out_specs=pl.BlockSpec(memory_space=pl.ANY),
            out_shape=jax.ShapeDtypeStruct((n, 2, part, d), BF16),
            scratch_shapes=[pltpu.VMEM((2, rows, d), BF16)] * (2 * STEP)
            + [
                pltpu.VMEM((STEP, 2 * queries, 2 * d), BF16),
                pltpu.VMEM((2, 2, GROUP, rows // 2), F32),
                pltpu.VMEM((GROUP, 128), F32),
                pltpu.VMEM((queries, queries), BF16),
                pltpu.VMEM((part, part), BF16),
                pltpu.VMEM((batches, STEP, 2, part, d), BF16),
                pltpu.VMEM((batches, STEP, 8, 128), F32),
                pltpu.VMEM((batches + 2, devices, part, d), BF16),
                pltpu.VMEM((batches + 2, devices, 8, 128), F32),
                pltpu.VMEM((batches + 2, part, d), BF16),
                dma((STEP, 2)),
                dma((STEP, 2)),
                dma((batches, devices)),
                dma((batches, devices)),
                dma((batches, devices)),
                dma((batches, devices)),
                dma((batches, devices)),
                dma((batches, devices)),
                dma((batches,)),
            ],
            compiler_params=pltpu.CompilerParams(
                collective_id=0, has_side_effects=True, vmem_limit_bytes=62 << 20
            ),
            name="attend",
        )(q, k.reshape(n, rows, d), v.reshape(n, rows, d))
        return out.reshape(q.shape)

    return jax.shard_map(
        step,
        mesh=mesh,
        in_specs=(P("dp", None, None), P("dp", "sp", None, None), P("dp", "sp", None, None)),
        out_specs=P("dp", None, None),
        check_vma=False,
    )
```
